32 devices in a mesh: rep: 4 (over z), row: 4 (over x, core), col: 2 (over y).
Axes of the slice: x: 2, y: 2, z: 4, core: 2. Of those that a mesh axis runs over, the one named last changes fastest.
Arguments:
- grad_parts: bfloat16 [4, 16384, 6144], P('rep', ('row', 'col')), may hold values from -0.03125 to 0.03125, as said below
- statistic: float32 [6144, 6144], P('row', 'col'), may hold values from -150 to 150, as said below
Outputs:
- gram_matrix: float32 [6144, 6144], P('row', 'col')
- statistic_next: float32 [6144, 6144], P('row', 'col')
The draws below stay inside these ranges and needn't reach their ends.
Inputs may be any that keep to these rules, and one draw needn't show every extreme that they name: Every entry of grad_parts has a magnitude between 2^-10 and 2^-5. statistic is symmetric and positive definite.
All inputs are finite; a program needn't handle non-finite values.
Results may differ from the reference program's by a relative error of at most 0.008.
Values may be sent and summed in bfloat16 or wider, within the bound.
A program may use at most 192 MiB of HBM per device.

```python
import math
import jax
import jax.numpy as jnp
from jax import lax

D = 6144
HID = 16384
N_REP = 4


def draw_grad_parts(key, part):
    key_sign = jax.random.fold_in(key, 41)
    key_level = jax.random.fold_in(key, 53)
    signs = jnp.where(jax.random.bernoulli(key_sign, 0.5, (N_REP, HID, D)), 1.0, -1.0).astype(jnp.float32)
    level = jax.random.uniform(key_level, (N_REP, HID, D), jnp.float32, -10.0, -5.0)
    return (signs * jnp.exp2(level)).astype(jnp.bfloat16)


def draw_statistic(key, part):
    key_factor = jax.random.fold_in(key, 11)
    key_ridge = jax.random.fold_in(key, 23)
    factor = jax.random.truncated_normal(key_factor, -3.0, 3.0, (D, D), jnp.float32) * (2.0 / math.sqrt(D))
    crossed = jnp.dot(factor.T, factor, precision=lax.Precision.HIGHEST)
    crossed = 0.5 * (crossed + crossed.T)
    ridge = jax.random.uniform(key_ridge, (D,), jnp.float32, 0.25, 1.0)
    return crossed + jnp.diag(ridge)


def setup_inputs(seed: int = 0) -> dict:
    seeds = jax.random.split(jax.random.key(seed), 3)
    grad_parts = draw_grad_parts(jax.random.fold_in(seeds[2], 71), 0)
    statistic = draw_statistic(jax.random.fold_in(seeds[2], 71), 0)
    return {"grad_parts": grad_parts, "statistic": statistic}


def reference(grad_parts, statistic):
    summed = jnp.sum(grad_parts.astype(jnp.float32), axis=0).astype(jnp.bfloat16)
    summed = lax.optimization_barrier(summed)
    summed_f32 = summed.astype(jnp.float32)
    product = jnp.dot(summed_f32.T, summed_f32, precision=lax.Precision.HIGHEST)
    gram_full = 0.5 * (product + product.T)
    statistic_next = 0.95 * statistic + 0.05 * gram_full
    return gram_full, statistic_next
```

```python
import jax
import jax.numpy as jnp
from jax import lax
from jax.sharding import PartitionSpec as P


SHARES = (8, 5, 3)


def masks(axis):
    size = lax.axis_size(axis)
    steps = []
    bit = size // 2
    while bit:
        steps.append((axis, bit, size))
        bit //= 2
    return steps


def double(block, step):
    axis, bit, size = step
    other = lax.ppermute(block, axis, [(i, i ^ bit) for i in range(size)])
    return jnp.concatenate([block, other], axis=0)


def plane_gather(block):
    row_steps, col_steps = masks("row"), masks("col")
    half = block.shape[0] // 2
    first, second = block[:half], block[half:]
    for step in col_steps + row_steps:
        first = double(first, step)
    for step in row_steps[:-1] + col_steps + row_steps[-1:]:
        second = double(second, step)
    return jnp.concatenate([first, second], axis=0)


def shards(grad_parts, statistic):
    own = grad_parts[0]
    rows, _ = own.shape
    tile_rows, tile_cols = statistic.shape
    row_start = lax.axis_index("row") * tile_rows
    col_start = lax.axis_index("col") * tile_cols
    unit = rows // sum(SHARES)

    summed, start = [], 0
    for share in SHARES:
        chunk = lax.slice_in_dim(own, start, start + share * unit, axis=0)
        start += share * unit
        summed.append(lax.psum_scatter(chunk, "rep", scatter_dimension=0, tiled=True))

    bands = 2
    band = tile_rows // bands
    totals = [None] * bands
    for block in summed:
        gathered = plane_gather(block)
        right = lax.dynamic_slice_in_dim(gathered, col_start, tile_cols, axis=1)
        for b in range(bands):
            left = lax.dynamic_slice_in_dim(gathered, row_start + b * band, band, axis=1)
            part = lax.dot_general(
                left, right, (((0,), (0,)), ((), ())), preferred_element_type=jnp.float32
            )
            totals[b] = part if totals[b] is None else totals[b] + part

    grams = []
    for total in totals:
        piece = lax.psum_scatter(total.astype(jnp.bfloat16), "rep", scatter_dimension=0, tiled=True)
        grams.append(lax.all_gather(piece, "rep", axis=0, tiled=True))
    gram_tile = jnp.concatenate(grams, axis=0).astype(jnp.float32)
    return (gram_tile, 0.95 * statistic + 0.05 * gram_tile)


def solution(mesh):
    return jax.shard_map(
        shards,
        mesh=mesh,
        in_specs=(P("rep", ("row", "col"), None), P("row", "col")),
        out_specs=(P("row", "col"), P("row", "col")),
        check_vma=False,
    )
```
